32 devices in a mesh: row: 4 (over y, x), col: 8 (over z, core).
Axes of the slice: x: 2, y: 2, z: 4, core: 2. Of those that a mesh axis runs over, the one named last changes fastest.
Arguments:
- trial: bfloat16 [2, 512, 2048], P(None, 'row', 'col'), may hold values from -6 to 6
- val_energy: float32 [512], P('row'), may hold values from -1 to 0
- cond_energy: float32 [2048], P('col'), may hold values from 0.5 to 2
- val_orbitals: bfloat16 [512, 20480], P('col', 'row'), may hold values from -0.25 to 0.25
- cond_orbitals: bfloat16 [2048, 20480], P('row', 'col'), may hold values from -0.125 to 0.125
- screening: bfloat16 [20480, 20480], P('row', 'col'), may hold values from -0.29882812 to 0.29882812
Outputs:
- applied: float32 [2, 512, 2048], P(None, 'row', 'col')
The draws below stay inside these ranges and needn't reach their ends.
All inputs are finite; a program needn't handle non-finite values.
Results may differ from the reference program's by a relative error of at most 0.0028.
Values may be sent and summed in bfloat16 or wider, within the bound.
No kernel may reach another device: no remote copies, remote signals or barrier semaphores. Data moves between devices by JAX's collectives and lax.ppermute only.
A program may use at most 128 MiB of HBM per device.

```python
import math
import jax
import jax.numpy as jnp
from jax import lax

NV = 512
NC = 2048
NMU = 20480
VECTORS = 2
N_ROW = 4


def levels(own_key, shape, cuts, least, high):
    gain = 1.0
    for dim, shards_of in cuts:
        steps = jax.random.uniform(jax.random.fold_in(jax.random.fold_in(own_key, 6), dim), (shards_of,), jnp.float32, least / len(cuts), high / len(cuts))
        gain = gain * jnp.repeat(jnp.exp(steps), shape[dim] // shards_of).reshape((-1,) + (1,) * (len(shape) - 1 - dim))
    return gain


def gaussian(own_key, dims, spread, bound, cuts=(), held_as=jnp.bfloat16):
    result = spread * jax.random.normal(own_key, dims, jnp.float32)
    if cuts:
        result = result * levels(own_key, dims, cuts, -0.22, 0.18)
    return jnp.clip(result, -bound, bound).astype(held_as)


def setup_inputs(seed: int = 0) -> dict:
    splits = jax.random.split(jax.random.key(seed), 7)
    return {
        "trial": gaussian(splits[0], (VECTORS, NV, NC), 1.0, 6.0, ((1, 4), (2, 8))),
        "val_energy": jnp.clip(-1.0 + 1.0 * jax.random.uniform(splits[1], (NV,), jnp.float32) ** levels(splits[1], (NV,), ((0, 4),), -0.2, 0.2), -1.0, 0.0),
        "cond_energy": jnp.clip(jnp.exp(math.log(2.0) - 1.3862944 * jax.random.uniform(splits[2], (NC,), jnp.float32) ** levels(splits[2], (NC,), ((0, 8),), -0.2, 0.2)), 0.5, 2.0),
        "val_orbitals": gaussian(splits[3], (NV, NMU), NV ** -0.5, 0.25, ((0, 8), (1, 4))),
        "cond_orbitals": gaussian(splits[4], (NC, NMU), NC ** -0.5, 0.125, ((0, 4), (1, 8))),
        "screening": gaussian(splits[5], (NMU, NMU), 0.05, 0.29882812, ((0, 4), (1, 8))),
    }


def reference(trial, val_energy, cond_energy, val_orbitals, cond_orbitals, screening):
    block = NMU // N_ROW
    encoded = [jnp.dot(trial[b], cond_orbitals, preferred_element_type=jnp.float32).astype(jnp.bfloat16) for b in range(VECTORS)]
    val_blocks = val_orbitals.reshape(NV, N_ROW, block).transpose(1, 0, 2)
    scr_blocks = screening.reshape(N_ROW, block, NMU)

    def step(carry, item):
        val_piece, scr_piece = item
        updated = []
        for b in range(VECTORS):
            moments = jnp.dot(val_piece.T, encoded[b], preferred_element_type=jnp.float32)
            screened = (scr_piece.astype(jnp.float32) * moments).astype(jnp.bfloat16)
            updated.append(carry[b] + jnp.dot(val_piece, screened, preferred_element_type=jnp.float32))
        return tuple(updated), None

    start = tuple(jnp.zeros((NV, NMU), jnp.float32) for b in range(VECTORS))
    halves, unused = lax.scan(step, start, (val_blocks, scr_blocks))
    kernels = [jnp.dot(halves[b].astype(jnp.bfloat16), cond_orbitals.T, preferred_element_type=jnp.float32) for b in range(VECTORS)]
    kernel = jnp.stack(kernels, axis=0)
    gaps = cond_energy[None, None, :] - val_energy[None, :, None]
    return gaps * trial.astype(jnp.float32) + kernel
```

```python
import jax
import jax.numpy as jnp
from jax import lax
from jax.experimental import pallas as pl
from jax.experimental.pallas import tpu as pltpu
from jax.sharding import PartitionSpec as P

F32 = jnp.float32
BF16 = jnp.bfloat16
VMEM_LIMIT = 60 << 20


def whole(shape):
    return pl.BlockSpec(shape, lambda i: (0,) * len(shape))


def smem():
    return pl.BlockSpec(memory_space=pltpu.SMEM)


def params():
    return pltpu.CompilerParams(vmem_limit_bytes=VMEM_LIMIT)


def divisor(size, most):
    best = 128
    for d in range(128, most + 1, 128):
        if size % d == 0:
            best = d
    return best


def prepare(where, own, other):
    n, (rows, m) = len(own), own[0].shape
    v = 2 * n * rows
    mb = divisor(m, 1280)

    def body(where_ref, *refs):
        out, flipped = refs[-2:]
        for d in range(n):
            out[pl.ds(pl.multiple_of(where_ref[2 * d], rows), rows), :] = refs[d][...]
            out[pl.ds(pl.multiple_of(where_ref[2 * d + 1], rows), rows), :] = refs[n + d][...]
        flipped[...] = out[...].T

    return pl.pallas_call(
        body,
        grid=(m // mb,),
        in_specs=[smem()] + [pl.BlockSpec((rows, mb), lambda i: (0, i))] * (2 * n),
        out_specs=[
            pl.BlockSpec((v, mb), lambda i: (0, i)),
            pl.BlockSpec((mb, v), lambda i: (i, 0)),
        ],
        out_shape=[jax.ShapeDtypeStruct((v, m), BF16), jax.ShapeDtypeStruct((m, v), BF16)],
        compiler_params=params(),
        name="prepare",
    )(where, *own, *other)


def encode(offsets, mine, other, pieces):
    v = mine.shape[0]
    width, nj = pieces[0].shape

    def body(off_ref, mine_ref, other_ref, *refs):
        out = refs[-1]
        for b, t_ref in enumerate((mine_ref, other_ref)):
            total = jnp.zeros((v, nj), F32)
            for i, piece in enumerate(refs[:-1]):
                lanes = pl.ds(pl.multiple_of(off_ref[i], width), width)
                total += jnp.dot(t_ref[:, lanes], piece[...], preferred_element_type=F32)
            out[b * v : (b + 1) * v, :] = total.astype(BF16)

    return pl.pallas_call(
        body,
        grid=(1,),
        in_specs=[smem(), whole(mine.shape), whole(other.shape)] + [whole(p.shape) for p in pieces],
        out_specs=whole((2 * v, nj)),
        out_shape=jax.ShapeDtypeStruct((2 * v, nj), BF16),
        compiler_params=params(),
        name="encode",
    )(offsets, mine, other, *pieces)


def screen(flipped, val, screening, enc, j):
    v, m = val.shape
    rows, nj = enc.shape
    mb = divisor(m, 1024)

    def body(vt_ref, v_ref, s_ref, e_ref, out, total):
        i = pl.program_id(0)

        @pl.when(i == 0)
        def _():
            total[...] = jnp.zeros_like(total)

        for b in range(rows // v):
            part = slice(b * v, (b + 1) * v)
            moments = jnp.dot(vt_ref[...], e_ref[part, :], preferred_element_type=F32)
            screened = (s_ref[...].astype(F32) * moments).astype(BF16)
            total[part, :] += jnp.dot(v_ref[...], screened, preferred_element_type=F32)

        @pl.when(i == pl.num_programs(0) - 1)
        def _():
            out[...] = total[...].astype(BF16)

    return pl.pallas_call(
        body,
        grid=(m // mb,),
        in_specs=[
            pl.BlockSpec((mb, v), lambda i: (i, 0)),
            pl.BlockSpec((v, mb), lambda i: (0, i)),
            pl.BlockSpec((mb, nj), lambda i: (i, j)),
            whole(enc.shape),
        ],
        out_specs=whole((rows, nj)),
        out_shape=jax.ShapeDtypeStruct((rows, nj), BF16),
        scratch_shapes=[pltpu.VMEM((rows, nj), F32)],
        compiler_params=params(),
        name="screen",
    )(flipped, val, screening, enc)


def decode(columns, halves, pieces, before, last):
    rows, nj = halves[0].shape
    width = pieces[0][0].shape[0]
    n = len(pieces[0]) // 2
    step = rows // 2
    types = (F32, BF16) if last else (F32, F32)

    def body(col_ref, *refs):
        h_refs = refs[: len(halves)]
        p_refs = refs[len(halves) : len(halves) + 2 * n * len(halves)]
        b_refs = refs[len(h_refs) + len(p_refs) : -2]
        outs = refs[-2:]
        for q in range(n):
            lanes = pl.ds(pl.multiple_of(col_ref[q], width), width)
            for side in range(2):
                total = b_refs[side][:, lanes] if b_refs else jnp.zeros((step, width), F32)
                for j, h_ref in enumerate(h_refs):
                    total += lax.dot_general(
                        h_ref[...],
                        p_refs[2 * n * j + 2 * q + side][...],
                        (((1,), (1,)), ((), ())),
                        preferred_element_type=F32,
                    )
                outs[side][:, lanes] = total.astype(outs[side].dtype)

    block = pl.BlockSpec((step, n * width), lambda i: (i, 0))
    flat = [p for chunk in pieces for p in chunk]
    return pl.pallas_call(
        body,
        grid=(2,),
        in_specs=[smem()]
        + [pl.BlockSpec((step, nj), lambda i: (i, 0))] * len(halves)
        + [whole(p.shape) for p in flat]
        + [block] * len(before),
        out_specs=[block, block],
        out_shape=[jax.ShapeDtypeStruct((rows, n * width), t) for t in types],
        compiler_params=params(),
        name="decode",
    )(columns, *halves, *flat, *before)


def after(x, *first):
    return lax.optimization_barrier((x,) + first)[0]


def pipelined(rows_on, cols_on):
    chips = cols_on // 2

    def by_row(x, q):
        return lax.ppermute(x, "row", [(i, i ^ q) for i in range(rows_on)])

    def by_core(x):
        return lax.ppermute(x, "col", [(i, i ^ 1) for i in range(cols_on)])

    def by_chip(x, d):
        return lax.ppermute(x, "col", [(i, (i + 2 * d) % cols_on) for i in range(cols_on)])

    def over_rows(x):
        h = x.shape[0] // 2
        got = {0: (x[:h], x[h:])}
        if rows_on == 4:
            a, b = by_row(x, 1), by_row(x, 2)
            got[1], got[2] = (a[:h], a[h:]), (b[:h], b[h:])
            got[3] = (by_row(b[:h], 1), by_row(a[h:], 2))
        else:
            for q in range(1, rows_on):
                a = by_row(x, q)
                got[q] = (a[:h], a[h:])
        return [got[q] for q in range(rows_on)]

    def local(trial, val_energy, cond_energy, val, cond, screening):
        vectors, v_own, c_own = trial.shape
        v, c = v_own * rows_on, c_own * cols_on
        k, n = val.shape[0], cond.shape[1]
        r = lax.axis_index("row")
        col = lax.axis_index("col")
        core, chip = col % 2, col // 2
        chunks = next(j for j in (5, 4, 2, 1) if n % (128 * j) == 0)
        nj = n // chunks

        def cut(x, at, size, axis):
            return lax.dynamic_slice_in_dim(x, at, size, axis)

        cond = jnp.concatenate([cut(cond, core * c_own, c_own, 0), cut(cond, (1 - core) * c_own, c_own, 0)], 0)
        own_chunks = [cond[:, j * nj : (j + 1) * nj] for j in range(chunks)]

        partner = by_core(lax.dynamic_index_in_dim(trial, 1 - core, 0, False))
        mine = lax.dynamic_index_in_dim(trial, core, 0, False)
        pair = jnp.where(
            core == 0, jnp.concatenate([mine, partner], 1), jnp.concatenate([partner, mine], 1)
        )
        lane = jnp.zeros((v_own, c), BF16)
        for d in range(chips):
            got = pair if d == 0 else by_chip(pair, d)
            lane = lax.dynamic_update_slice_in_dim(lane, got, (chip - d) % chips * 2 * c_own, 1)
        full = jnp.zeros((v, c), BF16)
        for q, (top, low) in enumerate(over_rows(lane)):
            full = lax.dynamic_update_slice_in_dim(full, top, (r ^ q) * v_own, 0)
            full = lax.dynamic_update_slice_in_dim(full, low, (r ^ q) * v_own + v_own // 2, 0)
        full_other = by_core(full)

        own_val = [val if d == 0 else by_chip(val, d) for d in range(chips)]
        other_val = [by_core(x) for x in own_val]
        where = jnp.stack(
            [2 * k * ((chip - d) % chips) + k * (core if s == 0 else 1 - core) for d in range(chips) for s in range(2)]
        )
        val_full, flipped = prepare(where, own_val, other_val)

        offsets = jnp.stack(
            [2 * c_own * (r ^ q) + c_own * (core if s == 0 else 1 - core) for q in range(rows_on) for s in range(2)]
        )
        columns = jnp.stack([c_own * (r ^ q) for q in range(rows_on)])
        pieces, halves = [], []
        for j in range(chunks):
            got = over_rows(own_chunks[j])
            pieces.append([p for pair_of in got for p in pair_of])
            enc = encode(offsets, full, full_other, pieces[j])
            halves.append(screen(flipped, val_full, screening, enc, j))
        before = ()
        if chunks > 1:
            before = decode(columns, halves[:-1], pieces[:-1], (), False)
        keep, give = decode(columns, halves[-1:], pieces[-1:], tuple(before), True)

        swapped = by_core(give).reshape(vectors, v, -1)[::-1].reshape(give.shape)
        keep = keep + swapped.astype(F32)
        send = keep.astype(BF16)
        total = cut(keep, chip * c_own, c_own, 1)
        for d in range(1, chips):
            total += by_chip(cut(send, (chip + d) % chips * c_own, c_own, 1), d).astype(F32)
        total = total.reshape(vectors, v, c_own)
        kernel = cut(total, r * v_own, v_own, 1)
        send = total.astype(BF16)
        for q in range(1, rows_on):
            kernel += by_row(cut(send, (r ^ q) * v_own, v_own, 1), q).astype(F32)
        kernel = jnp.where(core == 0, kernel, kernel[::-1])
        gaps = cond_energy[None, None, :] - val_energy[None, :, None]
        return gaps * trial.astype(F32) + kernel

    return local


def gathered(trial, val_energy, cond_energy, val_orbitals, cond_orbitals, screening):
    full_trial = lax.all_gather(trial, "col", axis=2, tiled=True)
    cond_full = lax.all_gather(cond_orbitals, "row", axis=0, tiled=True)
    val_full = lax.all_gather(val_orbitals, "col", axis=0, tiled=True)
    encoded = jnp.einsum("bvc,cn->bvn", full_trial, cond_full, preferred_element_type=F32).astype(BF16)
    scr_float = screening.astype(F32)
    pieces = []
    for b in range(trial.shape[0]):
        enc = lax.all_gather(encoded[b], "row", axis=0, tiled=True)
        moments = jnp.einsum("vm,vn->mn", val_full, enc, preferred_element_type=F32)
        screened = (scr_float * moments).astype(BF16)
        half = jnp.einsum("vm,mn->vn", val_full, screened, preferred_element_type=F32)
        half = lax.psum_scatter(half, "row", scatter_dimension=0, tiled=True).astype(BF16)
        part = jnp.einsum("vn,cn->vc", half, cond_full, preferred_element_type=F32)
        pieces.append(lax.psum_scatter(part, "col", scatter_dimension=1, tiled=True))
    gaps = cond_energy[None, None, :] - val_energy[None, :, None]
    return gaps * trial.astype(F32) + jnp.stack(pieces, axis=0)


def solution(mesh):
    rows_on, cols_on = mesh.shape["row"], mesh.shape["col"]
    placed = (
        P(None, "row", "col"),
        P("row"),
        P("col"),
        P("col", "row"),
        P("row", "col"),
        P("row", "col"),
    )

    def local(*args):
        trial = args[0]
        paired = cols_on == 2 * rows_on and trial.shape[0] == 2 and rows_on & (rows_on - 1) == 0
        aligned = trial.shape[2] % 128 == 0 and args[3].shape[0] % 16 == 0 and args[5].shape[1] % 128 == 0
        return (pipelined(rows_on, cols_on) if paired and aligned else gathered)(*args)

    return jax.shard_map(
        local, mesh=mesh, in_specs=placed, out_specs=P(None, "row", "col"), check_vma=False
    )
```

```python
import jax
import jax.numpy as jnp
from jax import lax
from jax.experimental import pallas as pl
from jax.experimental.pallas import tpu as pltpu
from jax.sharding import PartitionSpec as P


F32 = jnp.float32
BF16 = jnp.bfloat16
VMEM_LIMIT = 60 << 20


def whole(shape):
    return pl.BlockSpec(shape, lambda i: (0,) * len(shape))


def smem():
    return pl.BlockSpec(memory_space=pltpu.SMEM)


def params():
    return pltpu.CompilerParams(vmem_limit_bytes=VMEM_LIMIT)


def divisor(size, most):
    best = 128
    for d in range(128, most + 1, 128):
        if size % d == 0:
            best = d
    return best


def cost(flops, *arrays):
    moved = sum(x.size * x.dtype.itemsize for x in arrays)
    return pl.CostEstimate(flops=int(flops), bytes_accessed=int(moved), transcendentals=0)


def prepare(where, pieces, v):
    m = pieces[0].shape[1]
    mb = divisor(m, 1280)

    def body(where_ref, *refs):
        out = refs[-1]
        for i, piece in enumerate(refs[:-1]):
            rows = piece.shape[0]
            out[pl.ds(pl.multiple_of(where_ref[i], rows), rows), :] = piece[...]

    return pl.pallas_call(
        body,
        grid=(m // mb,),
        in_specs=[smem()] + [pl.BlockSpec((p.shape[0], mb), lambda i: (0, i)) for p in pieces],
        out_specs=pl.BlockSpec((v, mb), lambda i: (0, i)),
        out_shape=jax.ShapeDtypeStruct((v, m), BF16),
        compiler_params=params(),
        cost_estimate=cost(v * m * 800, *pieces),
        name="prepare",
    )(where, *pieces)


def encode(rows_at, core, mine, other, pieces):
    sides, v, lanes = mine.shape
    width, nj = pieces[0].shape
    n = len(pieces)

    def body(at_ref, core_ref, mine_ref, other_ref, *refs):
        hbm, (out, trial, cond, sems) = refs[:n], refs[n:]
        copies = [
            pltpu.make_async_copy(
                hbm[i], cond.at[pl.ds(pl.multiple_of(at_ref[i], width), width), :], sems.at[i]
            )
            for i in range(n)
        ]
        copies.append(pltpu.make_async_copy(mine_ref, trial.at[0], sems.at[n]))
        copies.append(pltpu.make_async_copy(other_ref, trial.at[1], sems.at[n + 1]))
        for copy in copies:
            copy.start()
        for copy in copies[:-1]:
            copy.wait()
        for b in range(2):
            if b == 1:
                copies[-1].wait()
            total = None
            for side in range(sides):
                part = jnp.dot(
                    trial[b, side], cond[side * lanes : (side + 1) * lanes, :], preferred_element_type=F32
                )
                total = part if total is None else total + part
            first = (core_ref[0] if b == 0 else 1 - core_ref[0]) * v
            out[pl.ds(pl.multiple_of(first, v), v), :] = total.astype(BF16)

    hbm = pl.BlockSpec(memory_space=pltpu.HBM)
    return pl.pallas_call(
        body,
        grid=(1,),
        in_specs=[smem(), smem()] + [hbm] * (n + 2),
        out_specs=whole((2 * v, nj)),
        out_shape=jax.ShapeDtypeStruct((2 * v, nj), BF16),
        scratch_shapes=[
            pltpu.VMEM((2, sides, v, lanes), BF16),
            pltpu.VMEM((sides * lanes, nj), BF16),
            pltpu.SemaphoreType.DMA((n + 2,)),
        ],
        compiler_params=params(),
        cost_estimate=cost(4 * v * sides * lanes * nj, mine, other, *pieces),
        name="encode",
    )(rows_at, core, mine, other, *pieces)


def screen(val, screening, enc, start):
    v, m = val.shape
    rows, nj = enc.shape
    mb = divisor(m, 1280)
    tile = divisor(nj, 512)

    def body(v_ref, s_ref, e_ref, out, total):
        i = pl.program_id(0)

        @pl.when(i == 0)
        def _():
            total[...] = jnp.zeros_like(total)

        for b in range(rows // v):
            for n in range(0, nj, tile):
                part = (slice(b * v, (b + 1) * v), slice(n, n + tile))
                moments = lax.dot_general(
                    v_ref[...], e_ref[part], (((0,), (0,)), ((), ())), preferred_element_type=F32
                )
                screened = (s_ref[:, n : n + tile].astype(F32) * moments).astype(BF16)
                total[part] += jnp.dot(v_ref[...], screened, preferred_element_type=F32)

        @pl.when(i == pl.num_programs(0) - 1)
        def _():
            out[...] = total[...].astype(BF16)

    return pl.pallas_call(
        body,
        grid=(m // mb,),
        in_specs=[
            pl.BlockSpec((v, mb), lambda i: (0, i)),
            pl.BlockSpec((mb, nj), lambda i: (i, start // nj)),
            whole(enc.shape),
        ],
        out_specs=whole((rows, nj)),
        out_shape=jax.ShapeDtypeStruct((rows, nj), BF16),
        scratch_shapes=[pltpu.VMEM((rows, nj), F32)],
        compiler_params=params(),
        cost_estimate=cost(4 * m * rows * nj, val, enc),
        name="screen",
    )(val, screening, enc)


def decode(rows_at, halves, pieces, b):
    v = halves[0].shape[0] // 2
    widths = [h.shape[1] for h in halves]
    width = pieces[0][0].shape[0]
    n, chunks = len(pieces[0]), len(halves)
    c = n * width

    def body(at_ref, *refs):
        h_refs = refs[:chunks]
        hbm = refs[chunks : chunks + n * chunks]
        outs = refs[chunks + n * chunks :][:2]
        held, sems = refs[-chunks - 1 : -1], refs[-1]
        copies = []
        for j in range(chunks):
            for i in range(n):
                at = pl.ds(pl.multiple_of(at_ref[i], width), width)
                copies.append(pltpu.make_async_copy(hbm[n * j + i], held[j].at[at, :], sems.at[i, j]))
                copies[-1].start()
        for side in range(2):
            total = None
            for j in range(chunks):
                if side == 0:
                    for copy in copies[n * j : n * (j + 1)]:
                        copy.wait()
                part = lax.dot_general(
                    held[j][side * (c // 2) : (side + 1) * (c // 2), :],
                    h_refs[j][...],
                    (((1,), (1,)), ((), ())),
                    preferred_element_type=F32,
                )
                total = part if total is None else total + part
            outs[side][...] = total.astype(outs[side].dtype)

    flat = [p for chunk in pieces for p in chunk]
    return pl.pallas_call(
        body,
        grid=(1,),
        in_specs=[smem()]
        + [pl.BlockSpec((v, nj), lambda i: (b, 0)) for nj in widths]
        + [pl.BlockSpec(memory_space=pltpu.HBM)] * len(flat),
        out_specs=[whole((c // 2, v))] * 2,
        out_shape=[jax.ShapeDtypeStruct((c // 2, v), t) for t in (F32, BF16)],
        scratch_shapes=[pltpu.VMEM((c, nj), BF16) for nj in widths] + [pltpu.SemaphoreType.DMA((n, chunks))],
        compiler_params=params(),
        cost_estimate=cost(2 * v * c * sum(widths), *flat),
        name="decode",
    )(rows_at, *halves, *flat)


def after(x, *first):
    return lax.optimization_barrier((x,) + first)[0]


def column_spans(n):
    unit = n // 5
    return ((4 * unit, unit), (0, 2 * unit), (2 * unit, 2 * unit))


def pipelined(rows_on, cols_on):
    chips = cols_on // 2

    def by_row(x, q):
        return lax.ppermute(x, "row", [(i, i ^ q) for i in range(rows_on)])

    def by_core(x):
        return lax.ppermute(x, "col", [(i, i ^ 1) for i in range(cols_on)])

    def by_chip(x, d):
        return lax.ppermute(x, "col", [(i, (i + 2 * d) % cols_on) for i in range(cols_on)])

    def near_rows(x):
        return [by_row(x, q) for q in range(1, 3 if rows_on == 4 else rows_on)]

    def over_rows(x, near):
        h = x.shape[0] // 2
        got = [(a[:h], a[h:]) for a in [x] + near]
        if rows_on == 4:
            got.append((by_row(got[2][0], 1), by_row(got[1][1], 2)))
        return got

    def local(trial, val_energy, cond_energy, val, cond, screening):
        _, v_own, c_own = trial.shape
        v, c = v_own * rows_on, c_own * cols_on
        k, n = val.shape[0], cond.shape[1]
        r = lax.axis_index("row")
        col = lax.axis_index("col")
        core, chip = col % 2, col // 2
        spans = column_spans(n)
        chunks = len(spans)

        def cut(x, at, size, axis):
            return lax.dynamic_slice_in_dim(x, at, size, axis)

        own = [cond[:, start : start + size] for start, size in spans]
        near, pieces = {}, []

        def ask(j, *first):
            if j < chunks:
                near[j] = near_rows(after(own[j], *first) if first else own[j])

        def ready(j):
            pieces.append([p for two in over_rows(own[j], near[j]) for p in two])

        partner = by_core(lax.dynamic_index_in_dim(trial, 1 - core, 0, False))
        ask(0)
        mine = lax.dynamic_index_in_dim(trial, core, 0, False)
        pair = jnp.where(core == 0, jnp.stack([mine, partner]), jnp.stack([partner, mine]))
        lane = jnp.zeros((2, v_own, c // 2), BF16)
        for d in range(chips):
            got = pair if d == 0 else by_chip(pair, d)
            lane = lax.dynamic_update_slice_in_dim(lane, got, (chip - d) % chips * c_own, 2)

        val_sent = after(val, lane)
        got_val = {d: by_chip(val_sent, d) for d in ((1, 3) if chips == 4 else range(1, chips))}
        placed = [(0, val)] + [(-d * 2 * k, x) for d, x in got_val.items()]
        if chips == 4:
            placed.append((-4 * k, by_chip(got_val[1][: k // 2], 1)))
            placed.append((-4 * k + k // 2, by_chip(got_val[3][k // 2 :], 3)))

        ready(0)
        near_trial = near_rows(lane)
        ask(1, *near_trial)
        full = jnp.zeros((2, v, c // 2), BF16)
        for q, two in enumerate(over_rows(lane, near_trial)):
            for side, got in enumerate(two):
                full = lax.dynamic_update_slice(full, got, (side, (r ^ q) * v_own, 0))
        full_other = by_core(full)

        at = [(side, c_own * (r ^ q)) for q in range(rows_on) for side in range(2)]
        core_of = jnp.stack([core])
        in_order = jnp.stack([side * (c // 2) + x for side, x in at])
        own_first = jnp.stack([jnp.where(side == core, 0, c // 2) + x for side, x in at])

        enc = encode(in_order, core_of, full, full_other, pieces[0])
        where, all_val = [], []
        for at, x in placed:
            where += [(2 * k * chip + at + k * core) % v, (2 * k * chip + at + k * (1 - core)) % v]
            all_val += [x, by_core(x)]
        ready(1)
        ask(2, *near[1])
        val_full = prepare(after(jnp.stack(where), enc), all_val, v)

        halves = []
        for j in range(chunks):
            if j == 0:
                enc = after(enc, *near[1])
            if j == 1:
                ready(2)
                enc = after(enc, *near[2])
            halves.append(screen(val_full, screening, enc, spans[j][0]))
            if j + 1 < chunks:
                enc = encode(after(in_order, halves[j]), core_of, full, full_other, pieces[j + 1])

        keep, give = decode(own_first, halves, pieces, 0)
        total = keep + by_core(give).astype(F32)
        sent = total.astype(BF16)
        first = cut(total, chip * c_own, c_own, 0)
        parts = [by_chip(cut(sent, (chip + d) % chips * c_own, c_own, 0), d) for d in range(1, chips)]

        keep, give = decode(after(own_first, give), halves, pieces, 1)
        total = keep + by_core(give).astype(F32)
        sent = total.astype(BF16)
        second = cut(total, r * v_own, v_own, 1)
        for q in range(1, rows_on):
            second += by_row(cut(sent, (r ^ q) * v_own, v_own, 1), q).astype(F32)
        for part in parts:
            first += part.astype(F32)

        sent = second.astype(BF16)
        second = cut(second, chip * c_own, c_own, 0)
        for d in range(1, chips):
            second += by_chip(cut(sent, (chip + d) % chips * c_own, c_own, 0), d).astype(F32)
        sent = first.astype(BF16)
        first = cut(first, r * v_own, v_own, 1)
        for q in range(1, rows_on):
            first += by_row(cut(sent, (r ^ q) * v_own, v_own, 1), q).astype(F32)
        gaps = cond_energy[None, None, :] - val_energy[None, :, None]
        return gaps * trial.astype(F32) + jnp.stack([first.T, second.T], axis=0)

    return local


def gathered(trial, val_energy, cond_energy, val_orbitals, cond_orbitals, screening):
    full_trial = lax.all_gather(trial, "col", axis=2, tiled=True)
    cond_full = lax.all_gather(cond_orbitals, "row", axis=0, tiled=True)
    val_full = lax.all_gather(val_orbitals, "col", axis=0, tiled=True)
    encoded = jnp.einsum("bvc,cn->bvn", full_trial, cond_full, preferred_element_type=F32).astype(BF16)
    scr_float = screening.astype(F32)
    pieces = []
    for b in range(trial.shape[0]):
        enc = lax.all_gather(encoded[b], "row", axis=0, tiled=True)
        moments = jnp.einsum("vm,vn->mn", val_full, enc, preferred_element_type=F32)
        screened = (scr_float * moments).astype(BF16)
        half = jnp.einsum("vm,mn->vn", val_full, screened, preferred_element_type=F32)
        half = lax.psum_scatter(half, "row", scatter_dimension=0, tiled=True).astype(BF16)
        part = jnp.einsum("vn,cn->vc", half, cond_full, preferred_element_type=F32)
        pieces.append(lax.psum_scatter(part, "col", scatter_dimension=1, tiled=True))
    gaps = cond_energy[None, None, :] - val_energy[None, :, None]
    return gaps * trial.astype(F32) + jnp.stack(pieces, axis=0)


def solution(mesh):
    rows_on, cols_on = mesh.shape["row"], mesh.shape["col"]
    placed = (
        P(None, "row", "col"),
        P("row"),
        P("col"),
        P("col", "row"),
        P("row", "col"),
        P("row", "col"),
    )

    def local(*args):
        trial = args[0]
        paired = cols_on == 2 * rows_on and trial.shape[0] == 2 and rows_on & (rows_on - 1) == 0
        aligned = trial.shape[2] % 128 == 0 and args[3].shape[0] % 32 == 0 and args[5].shape[1] % 640 == 0
        return (pipelined(rows_on, cols_on) if paired and aligned else gathered)(*args)

    return jax.shard_map(
        local, mesh=mesh, in_specs=placed, out_specs=P(None, "row", "col"), check_vma=False
    )
```

```python
import jax
import jax.numpy as jnp
from jax import lax
from jax.experimental import pallas as pl
from jax.experimental.pallas import tpu as pltpu
from jax.sharding import PartitionSpec as P


F32 = jnp.float32
BF16 = jnp.bfloat16
VMEM_LIMIT = 60 << 20


def whole(shape):
    return pl.BlockSpec(shape, lambda i: (0,) * len(shape))


def smem():
    return pl.BlockSpec(memory_space=pltpu.SMEM)


def params():
    return pltpu.CompilerParams(vmem_limit_bytes=VMEM_LIMIT)


def divisor(size, most):
    best = 128
    for d in range(128, most + 1, 128):
        if size % d == 0:
            best = d
    return best


def cost(flops, *arrays):
    moved = sum(x.size * x.dtype.itemsize for x in arrays)
    return pl.CostEstimate(flops=int(flops), bytes_accessed=int(moved), transcendentals=0)


def prepare(where, pieces, v):
    m = pieces[0].shape[1]
    mb = divisor(m, 1280)

    def body(where_ref, *refs):
        out = refs[-1]
        for i, piece in enumerate(refs[:-1]):
            rows = piece.shape[0]
            out[pl.ds(pl.multiple_of(where_ref[i], rows), rows), :] = piece[...]

    return pl.pallas_call(
        body,
        grid=(m // mb,),
        in_specs=[smem()] + [pl.BlockSpec((p.shape[0], mb), lambda i: (0, i)) for p in pieces],
        out_specs=pl.BlockSpec((v, mb), lambda i: (0, i)),
        out_shape=jax.ShapeDtypeStruct((v, m), BF16),
        compiler_params=params(),
        cost_estimate=cost(v * m * 800, *pieces),
        name="prepare",
    )(where, *pieces)


def encode(rows_at, core, mine, other, blocks, plan):
    sides, v, lanes = mine.shape
    nj = blocks[0].shape[1]
    n = len(plan)
    width = sides * lanes // n

    def body(at_ref, core_ref, mine_ref, other_ref, *refs):
        hbm, (out, trial, cond, sems) = refs[: len(blocks)], refs[len(blocks) :]
        copies = [
            pltpu.make_async_copy(
                hbm[block].at[pl.ds(first, width), :],
                cond.at[pl.ds(pl.multiple_of(at_ref[i], width), width), :],
                sems.at[i],
            )
            for i, (block, first) in enumerate(plan)
        ]
        copies.append(pltpu.make_async_copy(mine_ref, trial.at[0], sems.at[n]))
        copies.append(pltpu.make_async_copy(other_ref, trial.at[1], sems.at[n + 1]))
        for copy in copies:
            copy.start()
        for copy in copies[:-1]:
            copy.wait()
        for b in range(2):
            if b == 1:
                copies[-1].wait()
            total = None
            for side in range(sides):
                part = jnp.dot(
                    trial[b, side], cond[side * lanes : (side + 1) * lanes, :], preferred_element_type=F32
                )
                total = part if total is None else total + part
            first = (core_ref[0] if b == 0 else 1 - core_ref[0]) * v
            out[pl.ds(pl.multiple_of(first, v), v), :] = total.astype(BF16)

    hbm = pl.BlockSpec(memory_space=pltpu.HBM)
    return pl.pallas_call(
        body,
        grid=(1,),
        in_specs=[smem(), smem()] + [hbm] * (len(blocks) + 2),
        out_specs=whole((2 * v, nj)),
        out_shape=jax.ShapeDtypeStruct((2 * v, nj), BF16),
        scratch_shapes=[
            pltpu.VMEM((2, sides, v, lanes), BF16),
            pltpu.VMEM((sides * lanes, nj), BF16),
            pltpu.SemaphoreType.DMA((n + 2,)),
        ],
        compiler_params=params(),
        cost_estimate=cost(4 * v * sides * lanes * nj, mine, other, *blocks),
        name="encode",
    )(rows_at, core, mine, other, *blocks)


def screen(val, screening, enc, start):
    v, m = val.shape
    rows, nj = enc.shape
    mb = divisor(m, 1280)
    tile = divisor(nj, 512)

    def body(v_ref, s_ref, e_ref, out, total):
        i = pl.program_id(0)

        @pl.when(i == 0)
        def _():
            total[...] = jnp.zeros_like(total)

        for b in range(rows // v):
            for n in range(0, nj, tile):
                part = (slice(b * v, (b + 1) * v), slice(n, n + tile))
                moments = lax.dot_general(
                    v_ref[...], e_ref[part], (((0,), (0,)), ((), ())), preferred_element_type=F32
                )
                screened = (s_ref[:, n : n + tile].astype(F32) * moments).astype(BF16)
                total[part] += jnp.dot(v_ref[...], screened, preferred_element_type=F32)

        @pl.when(i == pl.num_programs(0) - 1)
        def _():
            out[...] = total[...].astype(BF16)

    return pl.pallas_call(
        body,
        grid=(m // mb,),
        in_specs=[
            pl.BlockSpec((v, mb), lambda i: (0, i)),
            pl.BlockSpec((mb, nj), lambda i: (i, start // nj)),
            whole(enc.shape),
        ],
        out_specs=whole((rows, nj)),
        out_shape=jax.ShapeDtypeStruct((rows, nj), BF16),
        scratch_shapes=[pltpu.VMEM((rows, nj), F32)],
        compiler_params=params(),
        cost_estimate=cost(4 * m * rows * nj, val, enc),
        name="screen",
    )(val, screening, enc)


def decode(rows_at, halves, blocks, plan, b):
    v = halves[0].shape[0] // 2
    widths = [h.shape[1] for h in halves]
    held_by, n, chunks = len(blocks[0]), len(plan), len(halves)
    width = blocks[0][-1].shape[0] if plan[-1][1] == 0 else plan[-1][1]
    c = n * width

    def body(at_ref, *refs):
        h_refs = refs[:chunks]
        hbm = refs[chunks : chunks + held_by * chunks]
        outs = refs[chunks + held_by * chunks :][:2]
        held, sems = refs[-chunks - 1 : -1], refs[-1]
        copies = []
        for j in range(chunks):
            for i, (block, first) in enumerate(plan):
                at = pl.ds(pl.multiple_of(at_ref[i], width), width)
                piece = hbm[held_by * j + block].at[pl.ds(first, width), :]
                copies.append(pltpu.make_async_copy(piece, held[j].at[at, :], sems.at[i, j]))
                copies[-1].start()
        for side in range(2):
            total = None
            for j in range(chunks):
                if side == 0:
                    for copy in copies[n * j : n * (j + 1)]:
                        copy.wait()
                part = lax.dot_general(
                    held[j][side * (c // 2) : (side + 1) * (c // 2), :],
                    h_refs[j][...],
                    (((1,), (1,)), ((), ())),
                    preferred_element_type=F32,
                )
                total = part if total is None else total + part
            outs[side][...] = total.astype(outs[side].dtype)

    flat = [x for chunk in blocks for x in chunk]
    return pl.pallas_call(
        body,
        grid=(1,),
        in_specs=[smem()]
        + [pl.BlockSpec((v, nj), lambda i: (b, 0)) for nj in widths]
        + [pl.BlockSpec(memory_space=pltpu.HBM)] * len(flat),
        out_specs=[whole((c // 2, v))] * 2,
        out_shape=[jax.ShapeDtypeStruct((c // 2, v), t) for t in (F32, BF16)],
        scratch_shapes=[pltpu.VMEM((c, nj), BF16) for nj in widths] + [pltpu.SemaphoreType.DMA((n, chunks))],
        compiler_params=params(),
        cost_estimate=cost(2 * v * c * sum(widths), *flat),
        name="decode",
    )(rows_at, *halves, *flat)


def after(x, *first):
    return lax.optimization_barrier((x,) + first)[0]


def column_spans(n):
    unit = n // 5
    return ((4 * unit, unit), (0, 2 * unit), (2 * unit, 2 * unit))


def pipelined(rows_on, cols_on):
    chips = cols_on // 2

    def by_row(x, q):
        return lax.ppermute(x, "row", [(i, i ^ q) for i in range(rows_on)])

    def by_core(x):
        return lax.ppermute(x, "col", [(i, i ^ 1) for i in range(cols_on)])

    def by_chip(x, d):
        return lax.ppermute(x, "col", [(i, (i + 2 * d) % cols_on) for i in range(cols_on)])

    def near_rows(x):
        return [by_row(x, q) for q in range(1, 3 if rows_on == 4 else rows_on)]

    def over_rows(x, near):
        h = x.shape[0] // 2
        got = [(a[:h], a[h:]) for a in [x] + near]
        if rows_on == 4:
            got.append((by_row(got[2][0], 1), by_row(got[1][1], 2)))
        return got

    def local(trial, val_energy, cond_energy, val, cond, screening):
        _, v_own, c_own = trial.shape
        v, c = v_own * rows_on, c_own * cols_on
        k, n = val.shape[0], cond.shape[1]
        r = lax.axis_index("row")
        col = lax.axis_index("col")
        core, chip = col % 2, col // 2
        spans = column_spans(n)
        chunks = len(spans)

        def cut(x, at, size, axis):
            return lax.dynamic_slice_in_dim(x, at, size, axis)

        own = [cond[:, start : start + size] for start, size in spans]
        near, blocks = {}, []
        plan = [(q, side * c_own) for q in range(rows_on) for side in range(2)]
        if rows_on == 4:
            plan[-2:] = [(3, 0), (4, 0)]

        def ask(j, *first):
            if j < chunks:
                near[j] = near_rows(after(own[j], *first) if first else own[j])

        def ready(j):
            got = [own[j]] + near[j]
            if rows_on == 4:
                got.append(by_row(near[j][1][:c_own], 1))
                got.append(by_row(near[j][0][c_own:], 2))
            blocks.append(got)

        partner = by_core(lax.dynamic_index_in_dim(trial, 1 - core, 0, False))
        ask(0)
        mine = lax.dynamic_index_in_dim(trial, core, 0, False)
        pair = jnp.where(core == 0, jnp.stack([mine, partner]), jnp.stack([partner, mine]))
        lane = jnp.zeros((2, v_own, c // 2), BF16)
        for d in range(chips):
            got = pair if d == 0 else by_chip(pair, d)
            lane = lax.dynamic_update_slice_in_dim(lane, got, (chip - d) % chips * c_own, 2)

        val_sent = after(val, lane)
        got_val = {d: by_chip(val_sent, d) for d in ((1, 3) if chips == 4 else range(1, chips))}
        placed = [(0, val)] + [(-d * 2 * k, x) for d, x in got_val.items()]
        if chips == 4:
            placed.append((-4 * k, by_chip(got_val[1][: k // 2], 1)))
            placed.append((-4 * k + k // 2, by_chip(got_val[3][k // 2 :], 3)))

        ready(0)
        near_trial = near_rows(lane)
        ask(1, *near_trial)
        full = jnp.zeros((2, v, c // 2), BF16)
        for q, two in enumerate(over_rows(lane, near_trial)):
            for side, got in enumerate(two):
                full = lax.dynamic_update_slice(full, got, (side, (r ^ q) * v_own, 0))
        full_other = by_core(full)

        at = [(side, c_own * (r ^ q)) for q in range(rows_on) for side in range(2)]
        core_of = jnp.stack([core])
        in_order = jnp.stack([side * (c // 2) + x for side, x in at])
        own_first = jnp.stack([jnp.where(side == core, 0, c // 2) + x for side, x in at])

        enc = encode(in_order, core_of, full, full_other, blocks[0], plan)
        where, all_val = [], []
        for at, x in placed:
            where += [(2 * k * chip + at + k * core) % v, (2 * k * chip + at + k * (1 - core)) % v]
            all_val += [x, by_core(x)]
        ready(1)
        ask(2, *near[1])
        val_full = prepare(after(jnp.stack(where), enc), all_val, v)

        halves = []
        for j in range(chunks):
            if j == 0:
                enc = after(enc, *near[1])
            if j == 1:
                ready(2)
                enc = after(enc, *near[2])
            halves.append(screen(val_full, screening, enc, spans[j][0]))
            if j + 1 < chunks:
                enc = encode(after(in_order, halves[j]), core_of, full, full_other, blocks[j + 1], plan)

        keep, give = decode(own_first, halves, blocks, plan, 0)
        total = keep + by_core(give).astype(F32)
        sent = total.astype(BF16)
        first = cut(total, chip * c_own, c_own, 0)
        parts = [by_chip(cut(sent, (chip + d) % chips * c_own, c_own, 0), d) for d in range(1, chips)]

        keep, give = decode(after(own_first, give), halves, blocks, plan, 1)
        total = keep + by_core(give).astype(F32)
        sent = total.astype(BF16)
        second = cut(total, r * v_own, v_own, 1)
        for q in range(1, rows_on):
            second += by_row(cut(sent, (r ^ q) * v_own, v_own, 1), q).astype(F32)
        for part in parts:
            first += part.astype(F32)

        sent = second.astype(BF16)
        second = cut(second, chip * c_own, c_own, 0)
        for d in range(1, chips):
            second += by_chip(cut(sent, (chip + d) % chips * c_own, c_own, 0), d).astype(F32)
        sent = first.astype(BF16)
        first = cut(first, r * v_own, v_own, 1)
        for q in range(1, rows_on):
            first += by_row(cut(sent, (r ^ q) * v_own, v_own, 1), q).astype(F32)
        gaps = cond_energy[None, None, :] - val_energy[None, :, None]
        return gaps * trial.astype(F32) + jnp.stack([first.T, second.T], axis=0)

    return local


def gathered(trial, val_energy, cond_energy, val_orbitals, cond_orbitals, screening):
    full_trial = lax.all_gather(trial, "col", axis=2, tiled=True)
    cond_full = lax.all_gather(cond_orbitals, "row", axis=0, tiled=True)
    val_full = lax.all_gather(val_orbitals, "col", axis=0, tiled=True)
    encoded = jnp.einsum("bvc,cn->bvn", full_trial, cond_full, preferred_element_type=F32).astype(BF16)
    scr_float = screening.astype(F32)
    pieces = []
    for b in range(trial.shape[0]):
        enc = lax.all_gather(encoded[b], "row", axis=0, tiled=True)
        moments = jnp.einsum("vm,vn->mn", val_full, enc, preferred_element_type=F32)
        screened = (scr_float * moments).astype(BF16)
        half = jnp.einsum("vm,mn->vn", val_full, screened, preferred_element_type=F32)
        half = lax.psum_scatter(half, "row", scatter_dimension=0, tiled=True).astype(BF16)
        part = jnp.einsum("vn,cn->vc", half, cond_full, preferred_element_type=F32)
        pieces.append(lax.psum_scatter(part, "col", scatter_dimension=1, tiled=True))
    gaps = cond_energy[None, None, :] - val_energy[None, :, None]
    return gaps * trial.astype(F32) + jnp.stack(pieces, axis=0)


def solution(mesh):
    rows_on, cols_on = mesh.shape["row"], mesh.shape["col"]
    placed = (
        P(None, "row", "col"),
        P("row"),
        P("col"),
        P("col", "row"),
        P("row", "col"),
        P("row", "col"),
    )

    def local(*args):
        trial = args[0]
        paired = cols_on == 2 * rows_on and trial.shape[0] == 2 and rows_on & (rows_on - 1) == 0
        aligned = trial.shape[2] % 128 == 0 and args[3].shape[0] % 32 == 0 and args[5].shape[1] % 640 == 0
        return (pipelined(rows_on, cols_on) if paired and aligned else gathered)(*args)

    return jax.shard_map(
        local, mesh=mesh, in_specs=placed, out_specs=P(None, "row", "col"), check_vma=False
    )
```
